128 devices in a mesh: kx: 8 (over z, y_lo), ky: 8 (over y_hi, x), kz: 2 (over core).
Axes of the slice: x: 4, y: 4 (y_hi: 2, y_lo: 2; y = y_hi * 2 + y_lo), z: 4, core: 2. Of those that a mesh axis runs over, the one named last changes fastest.
Arguments:
- u_start: float32 [8, 8, 8, 2, 128, 128], P('kx', 'ky', 'kz'), may hold values from -1 to 1, as said below
- intersections: float32 [8, 8, 8, 12, 2, 128, 128], P('kx', 'ky', 'kz'), may hold values from -1.2 to 1.2, as said below
Outputs:
- u_final: float32 [8, 8, 8, 2, 128, 128], P('kx', 'ky', 'kz')
- centres: float32 [3, 3, 128], replicated
- spreads: float32 [3, 128], replicated
The draws below stay inside these ranges and needn't reach their ends.
Inputs may be any that keep to these rules, and one draw needn't show every extreme that they name: `u_start`: each U(k) is unitary up to float32 rounding and close to the identity: every diagonal entry of U(k) has magnitude 0.7 or more. `intersections`: every diagonal entry of every M(k,b) has magnitude 0.45 or more and a phase within 1.9 of zero.
All inputs are finite; a program needn't handle non-finite values.
Results may differ from the reference program's by a relative error of at most 0.0003.
Values sent between devices are 32-bit elements; how exact they have to be, the bound alone decides.
No kernel may reach another device: no remote copies, remote signals or barrier semaphores. Data moves between devices by JAX's collectives and lax.ppermute only.
A program may use at most 128 MiB of HBM per device.

```python
import jax
import jax.numpy as jnp
from jax import lax

NW = 128
NBV = 12
ITERS = 3
NKX = 8
NKY = 8
NKZ = 8


OFFSETS = ((1, 1, 0), (1, -1, 0), (-1, 1, 0), (-1, -1, 0), (1, 0, 1), (1, 0, -1), (-1, 0, 1), (-1, 0, -1), (0, 1, 1), (0, 1, -1), (0, -1, 1), (0, -1, -1))


PRECISE = lax.Precision.HIGHEST


def random_entries(seed_key, dims, spread):
    return jax.random.normal(seed_key, dims, jnp.float32) * spread


def matmul_drawn(left, right):
    return jnp.einsum('...ij,...jk->...ik', left, right, precision=PRECISE)


def draw_u_start(key, part):
    dims = (NKX, NKY, NKZ, NW, NW)
    raw_real = random_entries(jax.random.fold_in(key, 3), dims, 0.02)
    raw_imag = random_entries(jax.random.fold_in(key, 5), dims, 0.02)
    gen_real = raw_real - jnp.swapaxes(raw_real, -1, -2)
    gen_imag = raw_imag + jnp.swapaxes(raw_imag, -1, -2)
    identity = jnp.broadcast_to(jnp.eye(NW, dtype=jnp.float32), dims)
    term_real = identity
    term_imag = jnp.zeros(dims, jnp.float32)
    total_real = identity
    total_imag = jnp.zeros(dims, jnp.float32)
    for order in range(1, 13):
        next_real = (matmul_drawn(term_real, gen_real) - matmul_drawn(term_imag, gen_imag)) / order
        next_imag = (matmul_drawn(term_real, gen_imag) + matmul_drawn(term_imag, gen_real)) / order
        term_real = next_real
        term_imag = next_imag
        total_real = total_real + term_real
        total_imag = total_imag + term_imag
    return jnp.stack([total_real, total_imag], axis=3)


def draw_intersections(key, part):
    dims = (NKX, NKY, NKZ, NBV, NW, NW)
    centre_draw = jax.random.uniform(jax.random.fold_in(key, 11), (3, NW), jnp.float32, -1.0, 1.0)
    offset_table = jnp.array(OFFSETS, jnp.float32)
    coherent = jnp.dot(offset_table, centre_draw, precision=PRECISE)
    slope = 0.5 + (jnp.arange(NKX, dtype=jnp.float32) + 0.5) / NKX
    noise = jax.random.uniform(jax.random.fold_in(key, 13), (NKX, NKY, NKZ, NBV, NW), jnp.float32, -0.4, 0.4)
    phases = -0.5 * slope[:, None, None, None, None] * coherent[None, None, None] + noise
    magnitude = jax.random.uniform(jax.random.fold_in(key, 15), (NKX, NKY, NKZ, NBV, NW), jnp.float32, 0.6, 1.0)
    off_real = random_entries(jax.random.fold_in(key, 17), dims, 0.03)
    off_imag = random_entries(jax.random.fold_in(key, 19), dims, 0.03)
    identity = jnp.eye(NW, dtype=jnp.float32)
    outside = 1.0 - identity
    over_real = off_real * outside + identity * (magnitude * jnp.cos(phases))[..., None, :]
    over_imag = off_imag * outside + identity * (magnitude * jnp.sin(phases))[..., None, :]
    return jnp.stack([over_real, over_imag], axis=4)


def setup_inputs(seed: int = 0) -> dict:
    key_list = jax.random.split(jax.random.key(seed), 3)
    u_start = draw_u_start(jax.random.fold_in(key_list[2], 71), 0)
    intersections = draw_intersections(jax.random.fold_in(key_list[2], 71), 0)
    return dict(u_start=u_start, intersections=intersections)


OFFSETS = ((1, 1, 0), (1, -1, 0), (-1, 1, 0), (-1, -1, 0), (1, 0, 1), (1, 0, -1), (-1, 0, 1), (-1, 0, -1), (0, 1, 1), (0, 1, -1), (0, -1, 1), (0, -1, -1))
WEIGHT = 0.125
STEP_SIZE = 0.35
PRECISE = lax.Precision.HIGHEST


def matmul(left, right):
    return jnp.einsum('...ij,...jk->...ik', left, right, precision=PRECISE)


def adjoint_product(left, right):
    return jnp.einsum('...ji,...jk->...ik', left, right, precision=PRECISE)


def complex_product(left_real, left_imag, right_real, right_imag):
    return (matmul(left_real, right_real) - matmul(left_imag, right_imag),
            matmul(left_real, right_imag) + matmul(left_imag, right_real))


def reference(u_start, intersections):
    total_points = NKX * NKY * NKZ
    offset_table = jnp.array(OFFSETS, jnp.float32)
    identity = jnp.eye(NW, dtype=jnp.float32)
    unitary = u_start
    centre_list = []
    spread_list = []
    for iteration in range(ITERS):
        local_real = unitary[:, :, :, 0]
        local_imag = unitary[:, :, :, 1]
        records = []
        first_sums = jnp.zeros((3, NW), jnp.float32)
        second_sums = jnp.zeros((NW,), jnp.float32)
        for vector_index in range(NBV):
            offset = OFFSETS[vector_index]
            nearby = jnp.roll(unitary, (-offset[0], -offset[1], -offset[2]), axis=(0, 1, 2))
            intersection_real = intersections[:, :, :, vector_index, 0]
            intersection_imag = intersections[:, :, :, vector_index, 1]
            left_real = adjoint_product(local_real, intersection_real) + adjoint_product(local_imag, intersection_imag)
            left_imag = adjoint_product(local_real, intersection_imag) - adjoint_product(local_imag, intersection_real)
            turned_real, turned_imag = complex_product(left_real, left_imag, nearby[:, :, :, 0], nearby[:, :, :, 1])
            diagonal_real = jnp.diagonal(turned_real, axis1=-2, axis2=-1)
            diagonal_imag = jnp.diagonal(turned_imag, axis1=-2, axis2=-1)
            phases = jnp.arctan2(diagonal_imag, diagonal_real)
            magnitude = diagonal_real * diagonal_real + diagonal_imag * diagonal_imag
            first_sums = first_sums + WEIGHT * offset_table[vector_index][:, None] * jnp.sum(phases, axis=(0, 1, 2))[None, :]
            second_sums = second_sums + WEIGHT * jnp.sum(1.0 - magnitude + phases * phases, axis=(0, 1, 2))
            records.append((turned_real, turned_imag, diagonal_real, diagonal_imag, phases, magnitude))
        centres = -first_sums / total_points
        spreads = second_sums / total_points - jnp.sum(centres * centres, axis=0)
        centre_list.append(centres)
        spread_list.append(spreads)
        summed_real = jnp.zeros((NKX, NKY, NKZ, NW, NW), jnp.float32)
        summed_imag = jnp.zeros((NKX, NKY, NKZ, NW, NW), jnp.float32)
        for vector_index in range(NBV):
            turned_real, turned_imag, diagonal_real, diagonal_imag, phases, magnitude = records[vector_index]
            shifted = phases + jnp.sum(offset_table[vector_index][:, None] * centres, axis=0)
            scaled = (shifted / magnitude)[..., None, :]
            product_real = turned_real * diagonal_real[..., None, :] + turned_imag * diagonal_imag[..., None, :]
            product_imag = turned_imag * diagonal_real[..., None, :] - turned_real * diagonal_imag[..., None, :]
            summed_real = summed_real + (product_real - product_imag * scaled)
            summed_imag = summed_imag + (product_imag + product_real * scaled)
        gradient_real = 2.0 * WEIGHT * (summed_real - jnp.swapaxes(summed_real, -1, -2))
        gradient_imag = 2.0 * WEIGHT * (summed_imag + jnp.swapaxes(summed_imag, -1, -2))
        change_real = STEP_SIZE * gradient_real
        change_imag = STEP_SIZE * gradient_imag
        inner_real = 0.5 * identity + change_real / 6.0
        inner_imag = change_imag / 6.0
        middle_real, middle_imag = complex_product(change_real, change_imag, inner_real, inner_imag)
        middle_real = identity + middle_real
        exponent_real, exponent_imag = complex_product(change_real, change_imag, middle_real, middle_imag)
        exponent_real = identity + exponent_real
        update_real, update_imag = complex_product(local_real, local_imag, exponent_real, exponent_imag)
        unitary = jnp.stack([update_real, update_imag], axis=3)
    return unitary, jnp.stack(centre_list), jnp.stack(spread_list)
```

```python
import functools

import jax
import jax.numpy as jnp
from jax import lax
from jax.experimental import pallas as pl
from jax.experimental.pallas import tpu as pltpu
from jax.sharding import PartitionSpec as P

ITERS = 3
AXES = ("kx", "ky", "kz")
OFFSETS = (
    (1, 1, 0),
    (1, -1, 0),
    (-1, 1, 0),
    (-1, -1, 0),
    (1, 0, 1),
    (1, 0, -1),
    (-1, 0, 1),
    (-1, 0, -1),
    (0, 1, 1),
    (0, 1, -1),
    (0, -1, 1),
    (0, -1, -1),
)
WEIGHT = 0.125
STEP_SIZE = 0.35
HIGH = lax.Precision.HIGH
F32 = jnp.float32


def cdot(lr, li, rr, ri):
    n = lr.shape[0]
    left = jnp.concatenate([lr, li], axis=1)
    right = jnp.concatenate(
        [jnp.concatenate([rr, ri], axis=1), jnp.concatenate([-ri, rr], axis=1)], axis=0
    )
    out = lax.dot_general(
        left, right, (((1,), (0,)), ((), ())), precision=HIGH, preferred_element_type=F32
    )
    return out[:, :n], out[:, n:]


def iotas(n):
    return (
        lax.broadcasted_iota(jnp.int32, (n, n), 0),
        lax.broadcasted_iota(jnp.int32, (n, n), 1),
    )


def expm(s):
    n = s.shape[0]
    row, col = iotas(n)
    t = s.T
    xr = jnp.where(row > col, s, jnp.where(row < col, -t, 0.0))
    xi = jnp.where(row <= col, s, t)
    eye = jnp.where(row == col, 1.0, 0.0).astype(F32)
    ar, ai = cdot(xr, xi, 0.5 * eye + xr * (1.0 / 6.0), xi * (1.0 / 6.0))
    er, ei = cdot(xr, xi, eye + ar, ai)
    return eye + er, ei


VMEM = pl.BlockSpec(memory_space=pltpu.VMEM)


def flops(products):
    return pl.CostEstimate(
        flops=products * 3 * 8 * 128**3, bytes_accessed=products * 3 * 131072, transcendentals=0
    )


def in_vmem(kernel, outs, args, cost=0, scratch=()):
    return pl.pallas_call(
        kernel,
        in_specs=[VMEM] * len(args),
        out_specs=jax.tree.map(lambda _: VMEM, outs),
        out_shape=outs,
        scratch_shapes=scratch,
        cost_estimate=flops(cost) if cost else None,
        compiler_params=pltpu.CompilerParams(vmem_limit_bytes=8 << 20),
    )(*args)


def product(m_ref, u_ref, p_ref, d_ref, z, b, first, near):
    pr, pi = cdot(m_ref[z, first + b, 0], m_ref[z, first + b, 1], *near)
    p_ref[z, b, 0] = pr
    p_ref[z, b, 1] = pi
    ur = u_ref[z, 0]
    ui = u_ref[z, 1]
    d_ref[z, b, 0:1] = jnp.sum(ur * pr + ui * pi, axis=0, keepdims=True)
    d_ref[z, b, 1:2] = jnp.sum(ur * pi - ui * pr, axis=0, keepdims=True)


def axis_kernel(packed, first, m_ref, u_ref, *refs):
    near = refs[:3]
    p_ref, d_ref = refs[3:5]
    nz = m_ref.shape[0]
    if packed:
        for src, dst in zip(near, refs[5:]):
            for j, (er, ei) in enumerate([expm(src[j]) for j in range(src.shape[0])]):
                dst[j, 0] = er
                dst[j, 1] = ei
        near = refs[5:]

    def planes(z, carry):
        for b in range(4):
            side = b // 2
            slab, halo = near[side], near[2]
            if b % 2 == 0:
                inside = z < nz - 1
                here = jnp.where(inside, z + 1, nz - 1)
            else:
                inside = z > 0
                here = jnp.where(inside, z - 1, 0)
            other = 2 * side + b % 2
            product(
                m_ref,
                u_ref,
                p_ref,
                d_ref,
                z,
                b,
                first,
                [jnp.where(inside, slab[here, i], halo[other, i]) for i in range(2)],
            )
        return carry

    lax.fori_loop(0, nz, planes, 0)


def axis_products(m, first, unitary, near):
    packed = near[0].ndim == 3
    nz, _, _, n, _ = m.shape
    outs = (
        jax.ShapeDtypeStruct((nz, 4, 2, n, n), F32),
        jax.ShapeDtypeStruct((nz, 4, 2, n), F32),
    )
    return in_vmem(
        functools.partial(axis_kernel, packed, first),
        outs,
        (m, unitary, *near),
        4 * nz + 24 * packed,
        [pltpu.VMEM((a.shape[0], 2, n, n), F32) for a in near] if packed else (),
    )


def corner_kernel(packed, m_ref, u_ref, q_ref, r_ref, dx_ref, dy_ref, p_ref, d_ref, f_ref, s_ref):
    nz = m_ref.shape[0]

    def planes(z, carry):
        where = ((q_ref, z), (r_ref, z), (q_ref, nz + z), (r_ref, nz + z))
        if packed:
            near = [expm(ref[j]) for ref, j in where]
        else:
            near = [(ref[j, 0], ref[j, 1]) for ref, j in where]
        for b in range(4):
            product(m_ref, u_ref, p_ref, d_ref, z, b, 0, near[b])
        return carry

    lax.fori_loop(0, nz, planes, 0)
    first = [0.0, 0.0, 0.0]
    second = 0.0
    for g, ref in enumerate((d_ref, dx_ref, dy_ref)):
        for b in range(4):
            dr = ref[:, b, 0, :]
            di = ref[:, b, 1, :]
            phase = jnp.arctan2(di, dr)
            f_ref[:, g * 4 + b, :] = phase
            total = jnp.sum(phase, axis=0, keepdims=True)
            offset = OFFSETS[g * 4 + b]
            for c in range(3):
                if offset[c]:
                    first[c] = first[c] + offset[c] * total
            second = second + jnp.sum(
                1.0 - (dr * dr + di * di) + phase * phase, axis=0, keepdims=True
            )
    sums = jnp.concatenate([WEIGHT * s for s in (*first, second)], axis=0)

    def copies(i, carry):
        s_ref[i] = sums
        return carry

    lax.fori_loop(0, s_ref.shape[0], copies, 0, unroll=8)


def corner_products(m, unitary, near, dx, dy, count):
    packed = near[0].ndim == 3
    nz, _, _, n, _ = m.shape
    outs = (
        jax.ShapeDtypeStruct((nz, 4, 2, n, n), F32),
        jax.ShapeDtypeStruct((nz, 4, 2, n), F32),
        jax.ShapeDtypeStruct((nz, 12, n), F32),
        jax.ShapeDtypeStruct((count, 4, n), F32),
    )
    return in_vmem(
        functools.partial(corner_kernel, packed),
        outs,
        (m, unitary, *near, dx, dy),
        4 * nz + 32 * packed,
    )


def z_kernel(u_ref, p0_ref, p1_ref, p2_ref, d0_ref, d1_ref, d2_ref, phase_ref, z_ref):
    n = u_ref.shape[-1]

    def planes(z, carry):
        acc = [[jnp.zeros((n, n), F32), jnp.zeros((n, n), F32)] for _ in range(4)]
        for g, (p_ref, d_ref) in enumerate(((p0_ref, d0_ref), (p1_ref, d1_ref), (p2_ref, d2_ref))):
            for b in range(4):
                pr = p_ref[z, b, 0]
                pi = p_ref[z, b, 1]
                dr = d_ref[z, b, 0:1]
                di = d_ref[z, b, 1:2]
                mag = dr * dr + di * di
                t = phase_ref[z, g * 4 + b : g * 4 + b + 1] / mag
                ar = dr + di * t
                ai = dr * t - di
                br = di / mag
                bi = dr / mag
                acc[0][0] += pr * ar - pi * ai
                acc[0][1] += pr * ai + pi * ar
                vr = pr * br - pi * bi
                vi = pr * bi + pi * br
                offset = OFFSETS[g * 4 + b]
                for c in range(3):
                    if offset[c] == 1:
                        acc[c + 1][0] += vr
                        acc[c + 1][1] += vi
                    elif offset[c] == -1:
                        acc[c + 1][0] -= vr
                        acc[c + 1][1] -= vi
        utr = u_ref[z, 0].T
        uti = -u_ref[z, 1].T
        for j in range(4):
            zr, zi = cdot(utr, uti, acc[j][0], acc[j][1])
            z_ref[z, j, 0] = zr
            z_ref[z, j, 1] = zi
        return carry

    lax.fori_loop(0, u_ref.shape[0], planes, 0)


def combine_parts(unitary, p, d, phase):
    nz, _, n, _ = unitary.shape
    return in_vmem(
        z_kernel,
        jax.ShapeDtypeStruct((nz, 4, 2, n, n), F32),
        (unitary, *p, *d, phase),
        8 * nz,
    )


def generator(r_ref, z_ref, z):
    n = z_ref.shape[-1]
    wr = z_ref[z, 0, 0]
    wi = z_ref[z, 0, 1]
    for c in range(3):
        r = r_ref[c : c + 1]
        wr = wr + z_ref[z, c + 1, 0] * r
        wi = wi + z_ref[z, c + 1, 1] * r
    row, col = iotas(n)
    return (STEP_SIZE * 2.0 * WEIGHT) * jnp.where(row > col, wr - wr.T, wi + wi.T)


def step_kernel(r_ref, z_ref, o_ref):
    for z in range(z_ref.shape[0]):
        o_ref[z] = generator(r_ref, z_ref, z)


def step(centres, zs):
    nz, _, _, n, _ = zs.shape
    return in_vmem(step_kernel, jax.ShapeDtypeStruct((nz, n, n), F32), (centres, zs))


def update_kernel(s_ref, u_ref, o_ref):
    nz = u_ref.shape[0]
    near = [expm(s_ref[z]) for z in range(nz)]
    for z in range(nz):
        vr, vi = cdot(u_ref[z, 0], u_ref[z, 1], *near[z])
        o_ref[z, 0] = vr
        o_ref[z, 1] = vi


def update(packed, unitary):
    shape = jax.ShapeDtypeStruct(unitary.shape, F32)
    return in_vmem(update_kernel, shape, (packed, unitary), 3 * unitary.shape[0])


def finish_kernel(r_ref, z_ref, u_ref, o_ref):
    nz = u_ref.shape[0]
    near = [expm(generator(r_ref, z_ref, z)) for z in range(nz)]
    for z in range(nz):
        vr, vi = cdot(u_ref[z, 0], u_ref[z, 1], *near[z])
        o_ref[z, 0] = vr
        o_ref[z, 1] = vi


def finish(centres, zs, unitary):
    shape = jax.ShapeDtypeStruct(unitary.shape, F32)
    return in_vmem(finish_kernel, shape, (centres, zs, unitary), 3 * unitary.shape[0])


def shift(value, axis, by):
    count = lax.axis_size(axis)
    return lax.ppermute(value, axis, [(i, (i - by) % count) for i in range(count)])


def edges(plus, minus):
    nz = plus.shape[0]
    mine = jnp.stack([plus[0], plus[nz - 1], minus[0], minus[nz - 1]])
    return shift(mine, "kz", 1)


def exchange(slab):
    xp = shift(slab, "kx", 1)
    xm = shift(slab, "kx", -1)
    yp = shift(slab, "ky", 1)
    ym = shift(slab, "ky", -1)
    both = jnp.concatenate([xp, xm])
    cp = shift(both, "ky", 1)
    cm = shift(both, "ky", -1)
    return (xp, xm, edges(xp, xm)), (yp, ym, edges(yp, ym)), (cp, cm)


def body(u_start, intersections):
    shape = u_start.shape
    nz = shape[2]
    n = shape[-1]
    count = lax.axis_size(AXES)
    total_points = nz * count
    unitary = u_start.reshape((nz, 2, n, n))
    m = intersections.reshape((nz, 12, 2, n, n))
    pc, px, py = m, m, m
    first = (4, 8)
    sent = unitary
    centre_list = []
    spread_list = []
    for iteration in range(ITERS):
        near_x, near_y, near_c = exchange(sent)
        if iteration > 0:
            unitary = update(sent, unitary)
        px, dx = axis_products(px, first[0], unitary, near_x)
        py, dy = axis_products(py, first[1], unitary, near_y)
        pc, dc, phase, spread = corner_products(pc, unitary, near_c, dx, dy, count)
        first = (0, 0)
        total = jnp.sum(lax.all_to_all(spread, AXES, 0, 0, tiled=True), axis=0)
        zs = combine_parts(unitary, (pc, px, py), (dc, dx, dy), phase)
        centres = -total[:3] / total_points
        spreads = total[3] / total_points - jnp.sum(centres * centres, axis=0)
        centre_list.append(centres)
        spread_list.append(spreads)
        if iteration < ITERS - 1:
            sent = step(centres, zs)
        else:
            unitary = finish(centres, zs, unitary)
    return (unitary.reshape(shape), jnp.stack(centre_list), jnp.stack(spread_list))


def solution(mesh):
    return jax.shard_map(
        body,
        mesh=mesh,
        in_specs=(P(*AXES, None, None, None), P(*AXES, None, None, None, None)),
        out_specs=(P(*AXES, None, None, None), P(), P()),
        check_vma=False,
    )
```
